32 devices in a mesh: dp: 4 (over z), mp: 8 (over y, x, core).
Axes of the slice: x: 2, y: 2, z: 4, core: 2. Of those that a mesh axis runs over, the one named last changes fastest.
Arguments:
- activations: bfloat16 [6144, 8192], P('dp', 'mp'), may hold values from -6 to 6
- grad_output: bfloat16 [6144, 16384], P('dp', 'mp'), may hold values from -0.078125 to 0.078125
- holder_index: int32 [8, 32, 1], replicated, may hold values from 0 to 7; in each aligned block of 32 rows (0 to 31, 32 to 63, ..., all dimensions but the last counted through in order) at most 4 rows name the same one
- row_offset: int32 [8, 32], replicated, may hold values from 0 to 7
- column_offset: int32 [8, 32], replicated, may hold values from 0 to 15
- live_counts: int32 [8], replicated, may hold values from 1 to 32, as said below
Outputs:
- candidate_grads: float32 [8, 32, 128, 128], P('mp', 'dp')
The draws below stay inside these ranges and needn't reach their ends.
Inputs may be any that keep to these rules, and one draw needn't show every extreme that they name: In each owner's 32 slots at most 4 have the same holder_index, a bound that some block reaches. Slots from live_counts[o] on are unused; some owner uses all 32 slots.
All inputs are finite; a program needn't handle non-finite values.
Results may differ from the reference program's by a relative error of at most 0.0003.
Values may be sent and summed in bfloat16 or wider, within the bound.
No kernel may reach another device: no remote copies, remote signals or barrier semaphores. Data moves between devices by JAX's collectives and lax.ppermute only.
A program may use at most 192 MiB of HBM per device.

```python
import math
import jax
import jax.numpy as jnp
import numpy as np
from jax import lax

D = 8192
FFW = 16384
BLK = 128
CAND = 32
OWNERS = 8
TOKENS = 6144
PER_PEER = 4


def draw_live_counts(key, part):
    first_key, second_key = jax.random.split(jax.random.fold_in(key, 7))
    counted = jax.random.randint(first_key, (OWNERS,), 1, CAND + 1)
    fullest = jax.random.randint(second_key, (), 0, OWNERS)
    return jnp.where(jnp.arange(OWNERS) == fullest, CAND, counted).astype(jnp.int32)


def plant(entries, own_key, low, high):
    longest = entries.shape.index(max(entries.shape))
    spots = []
    for shift in (0, 1):
        where = [jax.random.randint(jax.random.fold_in(own_key, axis), (), 0, length) for axis, length in enumerate(entries.shape)]
        where[longest] = (where[longest] + shift) % entries.shape[longest]
        spots.append(tuple(where))
    return entries.at[spots[0]].set(low).at[spots[1]].set(high)


def level_of(rng, dims, pieces, smallest, top_value):
    def one(dim, shards_of):
        steps = jax.random.uniform(jax.random.fold_in(jax.random.fold_in(rng, 6), dim), (shards_of,), jnp.float32, smallest / len(pieces), top_value / len(pieces))
        return jnp.repeat(jnp.exp(steps), dims[dim] // shards_of).reshape((-1,) + (1,) * (len(dims) - dim - 1))

    loudness = one(*pieces[0])
    for cut in pieces[1:]:
        loudness = loudness * one(*cut)
    return loudness


def shared_out(own_key, own, number, rows, count, top, reach, lean):
    order = jax.random.permutation(own_key, count)
    heavy_load, ordinary = shares(count, rows * top, reach, lean, True), shares(count, rows * top, reach, lean, False)
    places = jnp.arange(count)

    def named(sizes, offset_by):
        used = int((sizes > 0).sum())
        fixed = max(1, used // 4)
        shifted = fixed + (places - fixed + offset_by * (used - fixed)) % max(1, count - fixed)
        return jnp.zeros((count,), jnp.int32).at[order[jnp.where(places < fixed, places, shifted)]].set(jnp.asarray(sizes, jnp.int32))

    sizes = jnp.where(number % 4 == 0, named(heavy_load, number // 4), named(ordinary, number - number // 4 - 1))
    mixed = jax.random.permutation(jax.random.fold_in(own, 3), count)
    donor, sink = mixed[0:count // 2 * 2:2], mixed[1:count // 2 * 2:2]
    margin = jnp.minimum(sizes[donor] - 1, reach - sizes[sink]) // 2
    margin = jnp.where((donor == order[0]) | (sink == order[0]) | (sizes[sink] == 0), 0, jnp.maximum(margin, 0))
    shifted = jax.random.randint(jax.random.fold_in(own, 4), (count // 2,), 0, 1 << 20) % (margin + 1)
    sizes = sizes.at[donor].add(-shifted).at[sink].add(shifted)
    items = jnp.searchsorted(jnp.cumsum(sizes), jnp.arange(rows * top), side="right").astype(jnp.int32)
    listing = items.reshape(top, rows).T
    listing = listing[jax.random.permutation(jax.random.fold_in(own, 1), rows)]
    offset_by = jax.random.randint(jax.random.fold_in(own, 2), (rows, 1), 0, top)
    return jnp.take_along_axis(listing, (jnp.arange(top)[None, :] + offset_by) % top, axis=1)


def shares(number_of, total, limit, slope, full):
    portions = [(1 << 20) // math.isqrt(rank ** slope) + 1 for rank in range(1, number_of + 1)]
    largest = limit if full else min(limit, max(-(-total // number_of), total * portions[0] // sum(portions)))
    least = 1 if total - largest >= number_of - 1 else 0
    counts, surplus = [largest] + [least] * (number_of - 1), total - largest - least * (number_of - 1)
    while surplus > 0:
        free = [i for i in range(1, number_of) if counts[i] < largest] or [i for i in range(1, number_of) if counts[i] < limit]
        pool, remaining = sum([portions[i] for i in free]), surplus
        for i in free:
            extra = min(limit - counts[i], max(1, remaining * portions[i] // pool), surplus)
            counts[i] = counts[i] + extra
            surplus = surplus - extra
    return np.array(counts)


def gaussian(stream_key, dims, spread, limit, shards=(), held_as=jnp.bfloat16):
    array = jax.random.normal(stream_key, dims, jnp.float32) * spread
    if len(shards) > 0:
        array = level_of(stream_key, dims, shards, -0.22, 0.18) * array
    return jnp.clip(array, min=-limit, max=limit).astype(held_as)


def setup_inputs(seed: int = 0) -> dict:
    seeds = jax.random.split(jax.random.key(seed), 7)
    activations = gaussian(seeds[0], (TOKENS, D), 1.0, 6.0, ((0, 4), (1, 8)))
    grad_output = gaussian(seeds[1], (TOKENS, FFW), TOKENS ** -0.5, 0.078125, ((0, 4), (1, 8)))
    holder_index_keys = jax.random.split(jax.random.fold_in(seeds[2], 1), OWNERS * CAND // CAND)
    holder_index_turns = jax.random.permutation(jax.random.fold_in(seeds[2], 3), OWNERS * CAND // CAND)
    holder_index = jax.vmap(lambda own, number: shared_out(jax.random.fold_in(seeds[2], 2), own, number, CAND, OWNERS, 1, PER_PEER, 2))(holder_index_keys, holder_index_turns).reshape((OWNERS, CAND, 1))
    row_offset = plant(jax.random.randint(seeds[3], (OWNERS, CAND), 0, D // (OWNERS * BLK)), jax.random.fold_in(seeds[3], 1), 0, (D // (OWNERS * BLK)) - 1).astype(jnp.int32)
    column_offset = plant(jax.random.randint(seeds[4], (OWNERS, CAND), 0, FFW // (OWNERS * BLK)), jax.random.fold_in(seeds[4], 1), 0, (FFW // (OWNERS * BLK)) - 1).astype(jnp.int32)
    live_counts = draw_live_counts(jax.random.fold_in(seeds[6], 71), 0)
    return {"activations": activations, "grad_output": grad_output, "holder_index": holder_index, "row_offset": row_offset, "column_offset": column_offset, "live_counts": live_counts}


def reference(activations, grad_output, holder_index, row_offset, column_offset, live_counts):
    per_holder = D // (OWNERS * BLK)
    per_owner = FFW // (OWNERS * BLK)
    row_ids = (holder_index[:, :, 0] * per_holder + row_offset).astype(jnp.int32)
    column_ids = (jnp.arange(OWNERS, dtype=jnp.int32)[:, None] * per_owner + column_offset).astype(jnp.int32)
    input_panels = activations.reshape(activations.shape[0], D // BLK, BLK)
    grad_panels = grad_output.reshape(grad_output.shape[0], FFW // BLK, BLK)
    is_used = jnp.arange(CAND, dtype=jnp.int32)[None, :] < live_counts[:, None]

    def one_owner(packed):
        rows_here, columns_here, used_here = packed
        picked_input = jnp.take(input_panels, rows_here, axis=1).astype(jnp.float32)
        picked_grad = jnp.take(grad_panels, columns_here, axis=1).astype(jnp.float32)
        blocks = jnp.einsum("tkr,tkc->krc", picked_input, picked_grad, precision=lax.Precision.HIGHEST)
        return jnp.where(used_here[:, None, None], blocks, jnp.zeros_like(blocks))

    return lax.map(one_owner, (row_ids, column_ids, is_used))
```

```python
import functools

import jax
import jax.numpy as jnp
from jax import lax
from jax.experimental import pallas as pl
from jax.experimental.pallas import tpu as pltpu
from jax.sharding import PartitionSpec as P


BLK = 128


def gathered_plan(activations, grad_output, holder_index, row_offset, column_offset, live_counts):
    owners = lax.axis_size("mp")
    my_index = lax.axis_index("mp")
    tokens_here = activations.shape[0]
    per_holder = activations.shape[1] // BLK
    per_owner = grad_output.shape[1] // BLK
    slot_count = row_offset.shape[1]
    my_holder = lax.dynamic_index_in_dim(holder_index[:, :, 0], my_index, 0, keepdims=False)
    my_offset = lax.dynamic_index_in_dim(row_offset, my_index, 0, keepdims=False)
    my_column = lax.dynamic_index_in_dim(column_offset, my_index, 0, keepdims=False)
    my_count = lax.dynamic_index_in_dim(live_counts, my_index, 0, keepdims=False)
    grad_panels = grad_output.reshape(tokens_here, per_owner, BLK)
    is_used = jnp.arange(slot_count, dtype=jnp.int32) < my_count
    gathered = lax.all_gather(activations, "mp", axis=1, tiled=True)
    input_panels = gathered.reshape(tokens_here, owners * per_holder, BLK)
    picked_input = jnp.take(input_panels, my_holder * per_holder + my_offset, axis=1)
    picked_grad = jnp.take(grad_panels, my_column, axis=1)
    blocks = jnp.einsum(
        "tkr,tkc->krc", picked_input, picked_grad, preferred_element_type=jnp.float32
    )
    blocks = jnp.where(is_used[:, None, None], blocks, jnp.zeros_like(blocks))
    summed = lax.psum_scatter(blocks, "dp", scatter_dimension=0, tiled=True)
    return summed[None]


def chosen(values, places):
    ids = jnp.arange(values.shape[1], dtype=jnp.int32)
    return jnp.sum(jnp.where(places[:, :, None] == ids, values[:, None, :], 0), axis=2)


def two_colors(by_holder, by_share, steps):
    slots = by_holder.shape[1]
    jump = chosen(by_share, by_holder)
    least = jnp.broadcast_to(jnp.arange(slots, dtype=jnp.int32), jump.shape)
    for _ in range(steps):
        both = chosen(least + jump * slots, jump)
        least, jump = jnp.minimum(least, both % slots), both // slots
    return (least > chosen(least, by_holder)).astype(jnp.int32)


def slot_ranks(held, slots, per):
    ids = jnp.arange(slots, dtype=jnp.int32)
    same = held[:, :, None] == held[:, None, :]
    spot = jnp.sum((same & (ids[None, :] < ids[:, None])).astype(jnp.int32), axis=2)
    near = ids[None, :] // per == ids[:, None] // per
    by_holder = jnp.sum(jnp.where(same & (spot[:, None, :] == spot[:, :, None] ^ 1), ids, 0), axis=2)
    by_share = jnp.broadcast_to(ids ^ 1, held.shape)
    first = two_colors(by_holder, by_share, (slots // 2 - 1).bit_length())
    alike = (first[:, None, :] == first[:, :, None]) & (ids[None, :] != ids[:, None])
    by_holder = jnp.sum(jnp.where(same & alike, ids, 0), axis=2)
    by_share = jnp.sum(jnp.where(near & alike, ids, 0), axis=2)
    return 2 * first + two_colors(by_holder, by_share, (slots // 4 - 1).bit_length())


def slot_tables(holder_index, row_offset, column_offset, live_counts, owners, per_holder):
    slots = row_offset.shape[1]
    per = slots // owners
    held = holder_index[:, :, 0]
    ids = jnp.arange(slots, dtype=jnp.int32)
    owner = jnp.arange(owners, dtype=jnp.int32)[:, None]
    flip = owner ^ held
    rank = slot_ranks(held, slots, per)
    codes = jnp.arange(owners * per_holder, dtype=jnp.int32)
    same = (held * per_holder + row_offset)[:, :, None] == codes[None, None, :]
    panels = jnp.arange(per_holder, dtype=jnp.int32)
    by_x = (flip == 2) | (flip == 3) | (flip == 7)
    by_y = (flip == 4) | (flip == 5) | (flip == 6)

    def positions(by):
        value = jnp.where(by & (rank < 2), 2 - rank, 0)
        wanted = jnp.max(jnp.where(same, value[:, :, None], 0), axis=(0, 1))
        key = (2 - wanted.reshape(owners, per_holder)) * per_holder + panels[None, :]
        return jnp.sum((key[:, None, :] < key[:, :, None]).astype(jnp.int32), axis=2)

    x_spot, y_spot = positions(by_x), positions(by_y)
    spots = jnp.concatenate([x_spot, y_spot], axis=0)
    order = jnp.sum((spots[:, None, :] == panels[None, :, None]).astype(jnp.int32) * panels, axis=2)
    spot = jnp.where(
        by_x[:, :, None], x_spot.reshape(-1)[None, None, :], y_spot.reshape(-1)[None, None, :]
    )
    spot = jnp.sum(jnp.where(same, spot, 0), axis=2)
    used = (ids[None, :] < live_counts[:, None]).astype(jnp.int32)
    packed = row_offset + (column_offset << 8) + (used << 16) + (spot << 17)
    hit = (held * per + rank)[:, None, :] == ids[None, :, None]
    words = jnp.sum(jnp.where(hit, packed[:, None, :], 0), axis=2)
    fills = (rank * (slots // per) + ids // per)[:, None, :] == ids[None, :, None]
    fillers = jnp.sum(jnp.where(fills, (flip + owners * (ids % per))[:, None, :], 0), axis=2)
    return words, order, fillers


def row_of(word):
    return word & 255


def column_of(word):
    return (word >> 8) & 255


def used_of(word):
    return (word >> 16) & 1


def spot_of(word):
    return word >> 17


ANY = pl.BlockSpec(memory_space=pl.ANY)
SMEM = pl.BlockSpec(memory_space=pltpu.SMEM)
VMEM = pl.BlockSpec(memory_space=pltpu.VMEM)
COST = 4 * 1536 * BLK * BLK


def work(count):
    return pl.CostEstimate(flops=int(count * COST), bytes_accessed=0, transcendentals=0)


def panel_copies(head, pieces, word, to, sems):
    spot = spot_of(word)
    column = pl.multiple_of(row_of(word) * BLK, BLK)
    cut = head.shape[0]
    rest = to.shape[0] - cut
    first = pltpu.make_async_copy(head.at[:, pl.ds(column, BLK)], to.at[pl.ds(0, cut)], sems.at[0])
    first.start()
    low = 0
    for piece in pieces:
        size = piece.shape[0]
        place = jnp.clip(spot - low, 0, size - 1)
        copy = pltpu.make_async_copy(piece.at[place], to.at[pl.ds(cut, rest)], sems.at[1])
        if len(pieces) == 1:
            copy.start()
        else:
            pl.when((spot >= low) & (spot < low + size))(copy.start)
        low += size
    return [first, pltpu.make_async_copy(pieces[0].at[0], to.at[pl.ds(cut, rest)], sems.at[1])]


def send_panels(me, order, shard, cut, low, high, owners, after=()):
    rest = shard.shape[0] - cut
    count = high - low

    def body(me_ref, order_ref, shard_ref, *refs):
        x_ref, y_ref, held, arrived, left = refs[-5:]
        moves = []
        for way, ref in enumerate((x_ref, y_ref)):
            for k in range(count):
                n = way * count + k
                start = pl.multiple_of(order_ref[me_ref[0] + way * owners, low + k] * BLK, BLK)
                source = shard_ref.at[pl.ds(cut, rest), pl.ds(start, BLK)]
                moves.append(
                    (
                        pltpu.make_async_copy(source, held.at[n], arrived.at[n]),
                        pltpu.make_async_copy(held.at[n], ref.at[k], left.at[n]),
                    )
                )
        for come, _ in moves:
            come.start()
        for come, go in moves:
            come.wait()
            go.start()
        for _, go in moves:
            go.wait()

    return pl.pallas_call(
        body,
        in_specs=[SMEM, SMEM, ANY] + [ANY] * len(after),
        out_specs=[ANY, ANY],
        out_shape=[jax.ShapeDtypeStruct((count, rest, BLK), shard.dtype)] * 2,
        scratch_shapes=[
            pltpu.VMEM((2 * count, rest, BLK), shard.dtype),
            pltpu.SemaphoreType.DMA((2 * count,)),
            pltpu.SemaphoreType.DMA((2 * count,)),
        ],
        cost_estimate=work(count),
        name="send_panels",
    )(me, order, shard, *after)


def pass_panels(me, words, x_source, y_source, ranks, per, tokens, after):
    flat = [*x_source, *y_source]
    parts = len(x_source)
    total = 2 * len(ranks)

    def body(me_ref, words_ref, *refs):
        ins, (held, arrived, left) = refs[: 2 * parts], refs[-3:]
        outs = refs[-3 - total : -3]
        me = me_ref[0]
        moves = []
        for n in range(total):
            source, owner_flip, holder_flip = ((ins[parts:], 2, 4), (ins[:parts], 5, 2))[n % 2]
            word = words_ref[me ^ owner_flip, (me ^ holder_flip) * per + ranks[n // 2]]
            come = panel_copies(source[0], source[1:], word, held.at[n], arrived.at[n])
            moves.append((come, pltpu.make_async_copy(held.at[n], outs[n].at[0], left.at[n])))
        for come, go in moves:
            for copy in come:
                copy.wait()
            go.start()
        for _, go in moves:
            go.wait()

    return pl.pallas_call(
        body,
        in_specs=[SMEM, SMEM] + [ANY] * (len(flat) + len(after)),
        out_specs=[ANY] * total,
        out_shape=[jax.ShapeDtypeStruct((1, tokens, BLK), flat[0].dtype)] * total,
        scratch_shapes=[
            pltpu.VMEM((total, tokens, BLK), flat[0].dtype),
            pltpu.SemaphoreType.DMA((total, 2)),
            pltpu.SemaphoreType.DMA((total,)),
        ],
        cost_estimate=work(total / 2),
        name="pass_panels",
    )(me, words, *flat, *after)


def product(panel, grad):
    return lax.dot_general(panel, grad, (((0,), (0,)), ((), ())), preferred_element_type=jnp.float32)


def grad_copy(grad_ref, word, to, sem):
    column = pl.multiple_of(column_of(word) * BLK, BLK)
    copy = pltpu.make_async_copy(grad_ref.at[:, pl.ds(column, BLK)], to, sem)
    copy.start()
    return copy


def block_grads(me, words, grad, sources, flips, ranks, per, after=()):
    count = len(ranks)
    tokens = grad.shape[0]
    total = len(flips) * count
    arrays = [array for source in sources for array in source]

    def body(me_ref, words_ref, *refs):
        out_ref, inputs, grads, input_sems, grad_sems = refs[-5:]
        grad_ref = refs[len(arrays)]
        me = me_ref[0]
        waits, lives = [], []
        at = 0
        for k, source in enumerate(sources):
            own = refs[at : at + len(source)]
            at += len(own)
            for r, rank in enumerate(ranks):
                n = k * count + r
                word = words_ref[me, (me ^ flips[k]) * per + rank]
                lives.append(used_of(word) > 0)
                copies = [grad_copy(grad_ref, word, grads.at[n], grad_sems.at[n])]
                if len(own) == 1:
                    row = pl.multiple_of(row_of(word) * BLK, BLK)
                    copy = pltpu.make_async_copy(
                        own[0].at[:, pl.ds(row, BLK)], inputs.at[n], input_sems.at[n, 0]
                    )
                    copy.start()
                    copies.append(copy)
                else:
                    copies += panel_copies(own[0], own[1:], word, inputs.at[n], input_sems.at[n])
                waits.append(copies)
        for n in range(total):
            for copy in waits[n]:
                copy.wait()
            block = product(inputs[n], grads[n])
            out_ref[n] = jnp.where(lives[n], block, jnp.zeros_like(block))

    return pl.pallas_call(
        body,
        in_specs=[SMEM, SMEM] + [ANY] * (len(arrays) + 1 + len(after)),
        out_specs=VMEM,
        out_shape=jax.ShapeDtypeStruct((total, BLK, BLK), jnp.float32),
        scratch_shapes=[
            pltpu.VMEM((total, tokens, BLK), grad.dtype),
            pltpu.VMEM((total, tokens, BLK), grad.dtype),
            pltpu.SemaphoreType.DMA((total, 2)),
            pltpu.SemaphoreType.DMA((total,)),
        ],
        cost_estimate=work(total),
        name="block_grads",
    )(me, words, *arrays, grad, *after)


def finish_rank(meta, words, fillers, grad, far, zero, near, near_step, near_at, rank, per, groups, owners, after=()):
    tokens = grad.shape[0]
    share = owners // groups

    def body(meta_ref, words_ref, fillers_ref, *refs):
        far_refs, grad_ref, zero_ref, near_ref = refs[:2], refs[2], refs[3], refs[4]
        outs = refs[-5 - groups : -5]
        inputs, grads, blocks, input_sems, grad_sems = refs[-5:]
        me, group = meta_ref[0], meta_ref[1]
        waits, lives = [], []
        for n in range(2):
            word = words_ref[me, (me ^ (6 + n)) * per + rank]
            lives.append(used_of(word) > 0)
            copy = pltpu.make_async_copy(far_refs[n].at[0], inputs.at[n], input_sems.at[n])
            copy.start()
            waits.append([copy, grad_copy(grad_ref, word, grads.at[n], grad_sems.at[n])])
        blocks[0] = zero_ref[rank]
        blocks[1] = zero_ref[per + rank]
        for n, flip in enumerate((2, 4, 3, 5)):
            blocks[flip] = near_ref[n * near_step + near_at]
        for n in range(2):
            for copy in waits[n]:
                copy.wait()
            block = product(inputs[n], grads[n])
            blocks[6 + n] = jnp.where(lives[n], block, jnp.zeros_like(block))
        for step, out in enumerate(outs):
            to = lax.rem(group + step, groups)
            for k in range(share):
                flip = lax.rem(fillers_ref[me, rank * owners + to * share + k], owners)
                out[k] = blocks[flip]

    return pl.pallas_call(
        body,
        in_specs=[SMEM, SMEM, SMEM, ANY, ANY, ANY, VMEM, VMEM] + [ANY] * len(after),
        out_specs=[VMEM] * groups,
        out_shape=[jax.ShapeDtypeStruct((share, BLK, BLK), jnp.float32)] * groups,
        scratch_shapes=[
            pltpu.VMEM((2, tokens, BLK), grad.dtype),
            pltpu.VMEM((2, tokens, BLK), grad.dtype),
            pltpu.VMEM((owners, BLK, BLK), jnp.float32),
            pltpu.SemaphoreType.DMA((2,)),
            pltpu.SemaphoreType.DMA((2,)),
        ],
        cost_estimate=work(2),
        name="finish_rank",
    )(meta, words, fillers, *far, grad, zero, near, *after)


def place_sums(meta, fillers, ranks, owners, per):
    groups = len(ranks[0])
    share = owners // groups

    def body(meta_ref, fillers_ref, *refs):
        out_ref = refs[-1]
        for r in range(len(ranks)):
            parts = refs[r * groups : (r + 1) * groups]
            for k in range(share):
                filler = fillers_ref[meta_ref[0], r * owners + meta_ref[1] * share + k]
                block = parts[0][k]
                for part in parts[1:]:
                    block = block + part[k]
                out_ref[k * per + filler // owners] = block

    flat = [part for parts in ranks for part in parts]
    return pl.pallas_call(
        body,
        in_specs=[SMEM, SMEM] + [VMEM] * len(flat),
        out_specs=VMEM,
        out_shape=jax.ShapeDtypeStruct((share * per, BLK, BLK), jnp.float32),
        cost_estimate=work(1),
        name="place_sums",
    )(meta, fillers, *flat)


def flipped(array, bits):
    count = lax.axis_size("mp")
    return lax.ppermute(array, "mp", [(i, i ^ bits) for i in range(count)])


def turned(array, step):
    count = lax.axis_size("dp")
    return lax.ppermute(array, "dp", [(i, (i + step) % count) for i in range(count)])


def square_plan(activations, grad_output, holder_index, row_offset, column_offset, live_counts):
    owners = lax.axis_size("mp")
    groups = lax.axis_size("dp")
    index = lax.axis_index("mp").astype(jnp.int32)
    group = lax.axis_index("dp").astype(jnp.int32)
    slots = row_offset.shape[1]
    per = slots // owners
    tokens = activations.shape[0]
    per_holder = activations.shape[1] // BLK
    cut = tokens // 3 // 16 * 16
    me = index.reshape(1)

    head = activations[:cut]
    x_head, y_head = flipped(head, 2), flipped(head, 4)
    twin = flipped(activations, 1)
    words, order, fillers = slot_tables(
        holder_index, row_offset, column_offset, live_counts, owners, per_holder
    )
    meta = jnp.stack([index, group])
    send = functools.partial(send_panels, me, order, activations, cut, owners=owners)
    grads = functools.partial(block_grads, me, words, grad_output, per=per)
    pass_on = functools.partial(pass_panels, me, words, per=per, tokens=tokens)
    finish = functools.partial(
        finish_rank, meta, words, fillers, grad_output, per=per, groups=groups, owners=owners
    )

    def finished(rank, near, near_step, near_at, after=()):
        parts = finish(far[rank], zero, near, near_step, near_at, rank, after=after)
        return parts, [parts[0]] + [turned(parts[step], step) for step in range(1, groups)]

    go = send(0, 3)
    x_0, y_0 = flipped(go[0], 2), flipped(go[1], 4)
    go = send(3, 6, after=go)
    x_1, y_1 = flipped(go[0], 2), flipped(go[1], 4)
    xt_head, yt_head = flipped(x_head, 1), flipped(y_head, 1)
    zero = grads([(activations,), (twin,)], [0, 1], list(range(per)), after=(*go, fillers, meta))

    far = []
    xt_0, yt_0 = flipped(x_0, 1), flipped(y_0, 1)
    go = pass_on((x_head, x_0), (y_head, y_0), [0], after=(zero,))
    far.append((flipped(go[0], 2), flipped(go[1], 5)))
    go = send(6, per_holder, after=go)
    x_2, y_2 = flipped(go[0], 2), flipped(go[1], 4)
    flips = [2, 4, 3, 5]
    near_0 = grads(
        [(x_head, x_0), (y_head, y_0), (xt_head, xt_0), (yt_head, yt_0)], flips, [0], after=go
    )
    xt_1, yt_1 = flipped(x_1, 1), flipped(y_1, 1)
    go = pass_on((x_head, x_0, x_1), (y_head, y_0, y_1), [1], after=(near_0,))
    far.append((flipped(go[0], 2), flipped(go[1], 5)))
    near_1 = grads(
        [(x_head, x_0, x_1), (y_head, y_0, y_1), (xt_head, xt_0, xt_1), (yt_head, yt_0, yt_1)],
        flips, [1], after=go,
    )
    parts, sum_0 = finished(0, near_0, 1, 0, after=(near_1,))
    xt_2, yt_2 = flipped(x_2, 1), flipped(y_2, 1)
    late = list(range(2, per))
    go = pass_on((x_head, x_0, x_1, x_2), (y_head, y_0, y_1, y_2), late, after=(parts[0],))
    for n, rank in enumerate(late):
        far.append((flipped(go[2 * n], 2), flipped(go[2 * n + 1], 5)))
    near_2 = grads(
        [(x_head, x_0, x_1, x_2), (y_head, y_0, y_1, y_2), (xt_head, xt_0, xt_1, xt_2), (yt_head, yt_0, yt_1, yt_2)],
        flips, late, after=go,
    )
    parts, sum_1 = finished(1, near_1, 1, 0, after=(near_2,))
    sums = [sum_0, sum_1]
    for n, rank in enumerate(late):
        parts, sum_n = finished(rank, near_2, len(late), n, after=(parts[0],))
        sums.append(sum_n)
    out = place_sums(meta, fillers, sums, owners, per)
    return out[None]


def solution(mesh):
    placed = (P("dp", "mp"), P("dp", "mp"), P(), P(), P(), P())
    square = (mesh.shape["mp"], mesh.shape["dp"]) == (8, 4)

    def body(*arrays):
        return (square_plan if square else gathered_plan)(*arrays)

    return jax.shard_map(
        body, mesh=mesh, in_specs=placed, out_specs=P("mp", "dp", None, None), check_vma=False
    )
```
